16 devices in a mesh: ez: 2 (over z), ey: 2 (over y), ex: 4 (over x, core).
Axes of the slice: x: 2, y: 2, z: 2, core: 2. Of those that a mesh axis runs over, the one named last changes fastest.
Arguments:
- tokens: bfloat16 [4096, 2048], P(('ez', 'ey', 'ex'))
- expert_ids: int32 [4096, 6], P(('ez', 'ey', 'ex'))
- gate_weights: float32 [4096, 6], P(('ez', 'ey', 'ex'))
- w_gate: bfloat16 [64, 2048, 1408], P(('ez', 'ey', 'ex'))
- w_up: bfloat16 [64, 2048, 1408], P(('ez', 'ey', 'ex'))
- w_down: bfloat16 [64, 1408, 2048], P(('ez', 'ey', 'ex'))
Outputs:
- output: bfloat16 [4096, 2048], P(('ez', 'ey', 'ex'))
All inputs are finite; a program needn't handle non-finite values.
Results may differ from the reference program's by a relative error of at most 0.00618276.
Values are sent between devices in bfloat16 or wider.
A program may use at most 1 GiB of HBM per device.

```python
import jax
import jax.numpy as jnp
from jax import lax

HIDDEN = 2048
EXPERT_FF = 1408
EXPERTS = 64
TOP_K = 6
TOKENS = 256
DEVICES = 16
TOTAL_TOK = DEVICES * TOKENS
LOCAL_EXPERTS = EXPERTS // DEVICES
PER_EXPERT = TOTAL_TOK * TOP_K // EXPERTS


def draw_routing(route_key):
    def one_source(src_key):
        key_first, key_rest, key_dev, key_order = jax.random.split(src_key, 4)
        first_block = jax.random.permutation(key_first, LOCAL_EXPERTS)
        rest_block = jax.random.permutation(key_rest, EXPERTS - LOCAL_EXPERTS) + LOCAL_EXPERTS
        positions = jnp.arange(EXPERTS)
        spaced = positions % DEVICES == 0
        first_idx = jnp.clip(positions // DEVICES, 0, LOCAL_EXPERTS - 1)
        rest_idx = jnp.clip(positions - positions // DEVICES - 1, 0, EXPERTS - LOCAL_EXPERTS - 1)
        expert_cycle = jnp.where(spaced, first_block[first_idx], rest_block[rest_idx])
        dev_perm = jax.random.permutation(key_dev, DEVICES)
        expert_cycle = dev_perm[expert_cycle // LOCAL_EXPERTS] * LOCAL_EXPERTS + expert_cycle % LOCAL_EXPERTS
        tok_perm = jax.random.permutation(key_order, TOKENS)
        slot_pos = tok_perm[:, None] * TOP_K + jnp.arange(TOP_K)[None, :]
        return expert_cycle[slot_pos % EXPERTS]
    src_keys = jax.random.split(route_key, DEVICES)
    return jax.vmap(one_source)(src_keys).reshape(TOTAL_TOK, TOP_K).astype(jnp.int32)


def setup_inputs(seed: int = 0) -> dict:
    root_key = jax.random.key(seed)
    key_tok, key_ids, key_gate, key_w1, key_w3, key_w2 = jax.random.split(root_key, 6)
    tokens = jax.random.normal(key_tok, (TOTAL_TOK, HIDDEN), jnp.float32).astype(jnp.bfloat16)
    expert_ids = draw_routing(key_ids)
    gate_logits = 0.7 * jax.random.normal(key_gate, (TOTAL_TOK, TOP_K), jnp.float32)
    gate_weights = jax.nn.softmax(gate_logits, axis=-1)
    w_gate = (jax.random.normal(key_w1, (EXPERTS, HIDDEN, EXPERT_FF), jnp.float32) * HIDDEN ** -0.5).astype(jnp.bfloat16)
    w_up = (jax.random.normal(key_w3, (EXPERTS, HIDDEN, EXPERT_FF), jnp.float32) * HIDDEN ** -0.5).astype(jnp.bfloat16)
    w_down = (jax.random.normal(key_w2, (EXPERTS, EXPERT_FF, HIDDEN), jnp.float32) * (2.0 * EXPERT_FF ** -0.5)).astype(jnp.bfloat16)
    return {"tokens": tokens, "expert_ids": expert_ids, "gate_weights": gate_weights, "w_gate": w_gate, "w_up": w_up, "w_down": w_down}


def reference(tokens, expert_ids, gate_weights, w_gate, w_up, w_down):
    sort_order = jnp.argsort(expert_ids.reshape(-1), stable=True)
    rows_by_expert = (sort_order // TOP_K).reshape(EXPERTS, PER_EXPERT)
    gates_by_expert = gate_weights.reshape(-1)[sort_order].reshape(EXPERTS, PER_EXPERT)

    def expert_step(acc_out, expert_args):
        row_ids, row_gates, gate_mat, up_mat, down_mat = expert_args
        x_rows = tokens[row_ids]
        gate_act = jnp.dot(x_rows, gate_mat, preferred_element_type=jnp.float32)
        up_act = jnp.dot(x_rows, up_mat, preferred_element_type=jnp.float32)
        hidden_act = (jax.nn.silu(gate_act) * up_act).astype(jnp.bfloat16)
        expert_out = jnp.dot(hidden_act, down_mat, preferred_element_type=jnp.float32)
        acc_out = acc_out.at[row_ids].add(expert_out * row_gates[:, None])
        return acc_out, None

    init_acc = jnp.zeros((TOTAL_TOK, HIDDEN), jnp.float32)
    moe_sum = lax.scan(expert_step, init_acc, (rows_by_expert, gates_by_expert, w_gate, w_up, w_down))[0]
    return (tokens.astype(jnp.float32) + moe_sum).astype(jnp.bfloat16)
```

```python
import jax
import jax.numpy as jnp
from jax import lax
from jax.experimental import pallas as pl
from jax.experimental.pallas import tpu as pltpu
from jax.sharding import PartitionSpec as P

MESH = pl.DeviceIdType.MESH
BF, F32 = jnp.bfloat16, jnp.float32
TOK, HID, FF, NE, NDEV = 256, 2048, 1408, 4, 16
CAP = 96
PER = 384
SLOTS = NDEV * CAP
WIN = 128
CW = 256
NC = HID // CW
PARTS = ((0, 96), (96, 80), (176, 80))
FULL = slice(None)


def layer_kernel(x_hbm, w1_hbm, w3_hbm, w2_hbm, l1_ref, l2_ref, t_ref, gp_ref, st_ref, out_hbm,
                 x_all, acc_a, acc_b, h_act, slots, og, w13, w2b, xres, st0, st1, st2,
                 ag_send, ag_recv, rs_send, rs_recv, d_send, d_recv, w13_sem, w2_sem, loc_sem, credit):
    ez, ey, ex = lax.axis_index("ez"), lax.axis_index("ey"), lax.axis_index("ex")
    core = ex % 2
    pos = (ex // 2, ey, ez)

    def device(p, c):
        return (p[2], p[1], p[0] * 2 + c)

    def nbr(axis):
        p = list(pos)
        p[axis] = 1 - p[axis]
        return device(p, core)

    partner = device(pos, 1 - core)

    def cols(h):
        return pl.ds(pl.multiple_of(h * CW, CW), CW)

    def blocks(sel, c, rows, h):
        return x_all.at[sel[2], sel[1], sel[0], c, rows, cols(h)]

    def rows_of(k):
        return pl.ds(PARTS[k][0], PARTS[k][1])

    def pick(k, full, flip=()):
        sel = []
        for axis in range(3):
            if axis in full:
                sel.append(FULL)
            else:
                sel.append(1 - pos[axis] if axis in flip else pos[axis])
        return sel

    def ag(h, k, kind):
        a = [(k + i) % 3 for i in range(3)]
        if kind == 3:
            ref, to = blocks(pick(k, (a[0], a[1])), core, rows_of(k), h), partner
        elif kind == 4:
            ref, to = blocks(pick(k, (a[0], a[1]), (a[2],)), core, rows_of(k), h), partner
        else:
            ref, to = blocks(pick(k, tuple(a[:kind])), core, rows_of(k), h), nbr(a[kind])
        return pltpu.make_async_remote_copy(ref, ref, ag_send.at[h, k, kind], ag_recv.at[h, k, kind], device_id=to, device_id_type=MESH)

    def rs(h, k, kind):
        a = [(k + 2 - i) % 3 for i in range(3)]
        free = tuple(a[kind + 1:])
        src = blocks(pick(k, free, (a[kind],)), core, rows_of(k), h)
        if kind == 0:
            dst = st0.at[h % 2, :, :, rows_of(k), :]
        elif kind == 1:
            dst = st1.at[h % 2, :, rows_of(k), :]
        else:
            dst = st2.at[h % 2, rows_of(k), :]
        return pltpu.make_async_remote_copy(src, dst, rs_send.at[h, k, kind], rs_recv.at[h, k, kind], device_id=nbr(a[kind]), device_id_type=MESH)

    def cross(h):
        ref = blocks((FULL, FULL, FULL), 1 - core, FULL, h)
        return pltpu.make_async_remote_copy(ref, ref, d_send.at[h], d_recv.at[h], device_id=partner, device_id_type=MESH)

    def w13_copy(i, j):
        e, h = i % NE, i // NE
        src = (w1_hbm, w3_hbm)[j].at[e, pl.ds(pl.multiple_of(h * CW, CW), CW), :]
        return pltpu.make_async_copy(src, w13.at[i % 3, j], w13_sem.at[i % 3, j])

    def w2_copy(i):
        e, h = i % NE, i // NE
        return pltpu.make_async_copy(w2_hbm.at[e, :, cols(h)], w2b.at[i % 3], w2_sem.at[i % 3])

    own = pltpu.make_async_copy(x_hbm, x_all.at[pos[2], pos[1], pos[0], core], loc_sem.at[0])
    own.start()
    res = pltpu.make_async_copy(x_hbm, xres, loc_sem.at[1])
    res.start()
    for i in range(2):
        for j in range(2):
            w13_copy(i, j).start()

    barrier = pltpu.get_barrier_semaphore()
    for to in (nbr(0), nbr(1), nbr(2), partner):
        pl.semaphore_signal(barrier, inc=1, device_id=to, device_id_type=MESH)
    own.wait()
    pl.semaphore_wait(barrier, 4)

    def start(h, kind):
        for k in range(3):
            ag(h, k, kind).start()

    def arrive(h, kind):
        for k in range(3):
            ag(h, k, kind).wait_recv()

    for h in range(4):
        start(h, 0)

    def zero(i, _):
        acc_a[pl.ds(i * 128, 128), :] = jnp.zeros((128, FF), F32)
        acc_b[pl.ds(i * 128, 128), :] = jnp.zeros((128, FF), F32)
        return 0
    lax.fori_loop(0, NE * PER // 128, zero, 0)

    for h in range(2):
        arrive(h, 0)
        start(h, 1)

    def compact(h):
        def body(s, _):
            blk = x_all[s // 8, (s // 4) % 2, (s // 2) % 2, s % 2, :, cols(h)]
            slots[pl.ds(pl.multiple_of(s * CAP, CAP), CAP), :] = jnp.dot(l1_ref[s], blk, preferred_element_type=F32).astype(BF)
            return 0
        lax.fori_loop(0, NDEV, body, 0)

    def expert_in(h, e):
        i = h * NE + e
        for j in range(2):
            w13_copy(i, j).wait()

        @pl.when(i + 2 < NC * NE)
        def _():
            for j in range(2):
                w13_copy(i + 2, j).start()
        rows = pl.ds(pl.multiple_of(e * PER, PER), PER)
        xe = jnp.dot(l2_ref[rows, :], slots[...], preferred_element_type=F32).astype(BF)
        acc_a[rows, :] += jnp.dot(xe, w13[i % 3, 0], preferred_element_type=F32)
        acc_b[rows, :] += jnp.dot(xe, w13[i % 3, 1], preferred_element_type=F32)

    def experts_in(h, lo, hi):
        def body(e, _):
            expert_in(h, e)
            return 0
        lax.fori_loop(lo, hi, body, 0)

    def step_in(h, _):
        @pl.when(h < NC)
        def _():
            arrive(h, 1)
            start(h, 2)
            start(h, 3)

        @pl.when(h >= 1)
        def _():
            arrive(h - 1, 3)
            arrive(h - 1, 4)
            compact(h - 1)
            experts_in(h - 1, 0, 1)

        @pl.when(h + 2 < NC)
        def _():
            arrive(h + 2, 0)
            start(h + 2, 1)

        @pl.when(h + 4 < NC)
        def _():
            start(h + 4, 0)

        @pl.when(h >= 1)
        def _():
            experts_in(h - 1, 1, NE)

        @pl.when(h < NC)
        def _():
            arrive(h, 2)
            start(h, 4)
        return 0

    lax.fori_loop(0, NC + 1, step_in, 0)

    def drain(h, _):
        for k in range(3):
            for kind in range(5):
                ag(h, k, kind).wait_send()
        return 0
    lax.fori_loop(0, NC, drain, 0)
    pl.semaphore_signal(credit, inc=1, device_id=partner, device_id_type=MESH)
    for i in range(2):
        w2_copy(i).start()

    def activate(i, _):
        rows = pl.ds(pl.multiple_of(i * 32, 32), 32)
        a = acc_a[rows, :]
        h_act[rows, :] = (a * jax.nn.sigmoid(a) * acc_b[rows, :]).astype(BF)
        return 0
    lax.fori_loop(0, NE * PER // 32, activate, 0)
    res.wait()

    def expert_out(h):
        def body(e, _):
            i = h * NE + e
            w2_copy(i).wait()

            @pl.when(i + 2 < NC * NE)
            def _():
                w2_copy(i + 2).start()
            rows = pl.ds(pl.multiple_of(e * PER, PER), PER)
            o = jnp.dot(h_act[rows, :], w2b[i % 3], preferred_element_type=F32) * gp_ref[rows, :]
            high = o.astype(BF)
            tiles = pl.ds(e * (PER // 16), PER // 16)
            og[0, tiles] = high.reshape(PER // 16, 16, CW)
            og[1, tiles] = (o - high.astype(F32)).astype(BF).reshape(PER // 16, 16, CW)
            return 0
        lax.fori_loop(0, NE, body, 0)

    def spread(s):
        total = None
        for half in range(2):
            rhs = jnp.concatenate([og[half, pl.ds(st_ref[s * NE + e], WIN // 16)].reshape(WIN, CW) for e in range(NE)], axis=0)
            part = jnp.dot(t_ref[s], rhs, preferred_element_type=F32)
            total = part if total is None else total + part
        return total

    def spread_other(h):
        def body(j, _):
            x_all[j // 4, (j // 2) % 2, j % 2, 1 - core, :, cols(h)] = spread(j * 2 + 1 - core).astype(BF)
            return 0
        lax.fori_loop(0, NDEV // 2, body, 0)

    def spread_mine(h):
        def body(j, _):
            idx = (j // 4, (j // 2) % 2, j % 2, core, FULL, cols(h))
            x_all[idx] = (spread(j * 2 + core) + x_all[idx].astype(F32)).astype(BF)
            return 0
        lax.fori_loop(0, NDEV // 2, body, 0)

    def add_in(h, kind):
        for k in range(3):
            rs(h, k, kind).wait_recv()
            a = [(k + 2 - i) % 3 for i in range(3)]
            free = a[kind + 1:]
            rows = rows_of(k)
            if kind == 2:
                sel = pos
                mine = x_all[sel[2], sel[1], sel[0], core, rows, cols(h)].astype(F32) + st2[h % 2, rows, :].astype(F32)
                xres[rows, cols(h)] = (xres[rows, cols(h)].astype(F32) + mine).astype(BF)
                continue
            order = sorted(free, reverse=True)
            for n in range(2 ** len(order)):
                sel = list(pos)
                bits = [(n >> (len(order) - 1 - b)) & 1 for b in range(len(order))]
                for axis, bit in zip(order, bits):
                    sel[axis] = bit
                got = st0[h % 2, bits[0], bits[1], rows, :] if kind == 0 else st1[h % 2, bits[0], rows, :]
                idx = (sel[2], sel[1], sel[0], core, rows, cols(h))
                x_all[idx] = (x_all[idx].astype(F32) + got.astype(F32)).astype(BF)

    def step_out(h, _):
        @pl.when(h < NC)
        def _():
            expert_out(h)
            spread_other(h)

            @pl.when(h == 0)
            def _():
                pl.semaphore_wait(credit, 1)
            cross(h).start()

        @pl.when(jnp.logical_and(h >= 1, h < NC + 1))
        def _():
            add_in(h - 1, 0)
            for k in range(3):
                rs(h - 1, k, 1).start()

        @pl.when(h < NC)
        def _():
            cross(h).wait_recv()
            spread_mine(h)
            for k in range(3):
                rs(h, k, 0).start()

        @pl.when(jnp.logical_and(h >= 1, h < NC + 1))
        def _():
            add_in(h - 1, 1)
            for k in range(3):
                rs(h - 1, k, 2).start()

        @pl.when(h >= 2)
        def _():
            add_in(h - 2, 2)
        return 0

    lax.fori_loop(0, NC + 2, step_out, 0)

    def drain_out(h, _):
        for k in range(3):
            for kind in range(3):
                rs(h, k, kind).wait_send()
        cross(h).wait_send()
        return 0
    lax.fori_loop(0, NC, drain_out, 0)
    fin = pltpu.make_async_copy(xres, out_hbm, loc_sem.at[0])
    fin.start()
    fin.wait()


def route(ids, gates, ep_axes):
    dense_g = []
    for_all = jnp.arange(NDEV * NE)
    match = ids[:, :, None] == for_all[None, None, :]
    dense_g = jnp.sum(jnp.where(match, gates[:, :, None], 0.0), axis=1)
    dense_m = jnp.any(match, axis=1).astype(F32)
    both = jnp.stack([dense_g.T.reshape(NDEV, NE, TOK), dense_m.T.reshape(NDEV, NE, TOK)], axis=1)
    got = lax.all_to_all(both, ep_axes, 0, 0, tiled=True)
    gate, has = got[:, 0], got[:, 1] > 0.5
    hit = jnp.any(has, axis=1)
    slot = jnp.cumsum(hit.astype(jnp.int32), axis=1) - 1
    l1 = (hit[:, None, :] & (slot[:, None, :] == jnp.arange(CAP)[None, :, None]))
    within = jnp.cumsum(has.astype(jnp.int32), axis=2)
    count = within[:, :, -1]
    base = jnp.cumsum(count, axis=0) - count
    rank = base[:, :, None] + within - 1
    begin = jnp.minimum(base // 16 * 16, PER - WIN)
    l1f = l1.astype(F32)
    pick = lambda v: jnp.sum(jnp.where(l1[:, None, :, :], v[:, :, None, :], 0), axis=-1)
    slot_rank = pick(jnp.where(has, rank + 1, 0)) - 1
    l2 = slot_rank.transpose(1, 0, 2).reshape(NE, 1, SLOTS) == jnp.arange(PER)[None, :, None]
    slot_gate = pick(gate).transpose(1, 0, 2).reshape(NE, 1, SLOTS)
    gp = jnp.sum(jnp.where(l2, slot_gate, 0.0), axis=2).reshape(NE * PER, 1)
    at = jnp.where(has, rank - begin[:, :, None], -1).transpose(0, 2, 1)
    t = (at[:, :, :, None] == jnp.arange(WIN)[None, None, None, :]).reshape(NDEV, TOK, NE * WIN)
    return l1.astype(BF), l2.reshape(NE * PER, SLOTS).astype(BF), t.astype(BF), gp, (begin // 16 + jnp.arange(NE)[None, :] * (PER // 16)).reshape(-1).astype(jnp.int32)


def solution(mesh):
    ep_axes = tuple(mesh.axis_names)
    row_spec, w_spec = P(ep_axes, None), P(ep_axes, None, None)
    vmem, anyspace = pl.BlockSpec(memory_space=pltpu.VMEM), pl.BlockSpec(memory_space=pl.ANY)

    def local_layer(tokens, ids, gates, w1, w3, w2):
        l1, l2, t, gp, begin = route(ids, gates, ep_axes)
        return pl.pallas_call(
            layer_kernel,
            name="moe_layer",
            out_shape=jax.ShapeDtypeStruct((TOK, HID), BF),
            in_specs=[anyspace] * 4 + [vmem] * 4 + [pl.BlockSpec(memory_space=pltpu.SMEM)],
            out_specs=anyspace,
            scratch_shapes=[
                pltpu.VMEM((2, 2, 2, 2, TOK, HID), BF),
                pltpu.VMEM((NE * PER, FF), F32),
                pltpu.VMEM((NE * PER, FF), F32),
                pltpu.VMEM((NE * PER, FF), BF),
                pltpu.VMEM((SLOTS, CW), BF),
                pltpu.VMEM((2, NE * PER // 16, 16, CW), BF),
                pltpu.VMEM((3, 2, CW, FF), BF),
                pltpu.VMEM((3, FF, CW), BF),
                pltpu.VMEM((TOK, HID), BF),
                pltpu.VMEM((2, 2, 2, TOK, CW), BF),
                pltpu.VMEM((2, 2, TOK, CW), BF),
                pltpu.VMEM((2, TOK, CW), BF),
                pltpu.SemaphoreType.DMA((NC, 3, 5)),
                pltpu.SemaphoreType.DMA((NC, 3, 5)),
                pltpu.SemaphoreType.DMA((NC, 3, 3)),
                pltpu.SemaphoreType.DMA((NC, 3, 3)),
                pltpu.SemaphoreType.DMA((NC,)),
                pltpu.SemaphoreType.DMA((NC,)),
                pltpu.SemaphoreType.DMA((3, 2)),
                pltpu.SemaphoreType.DMA((3,)),
                pltpu.SemaphoreType.DMA((2,)),
                pltpu.SemaphoreType.REGULAR,
            ],
            compiler_params=pltpu.CompilerParams(collective_id=0, has_side_effects=True, vmem_limit_bytes=67_043_328),
        )(tokens, w1, w3, w2, l1, l2, t, gp, begin)

    return jax.shard_map(local_layer, mesh=mesh, in_specs=(row_spec, row_spec, row_spec, w_spec, w_spec, w_spec), out_specs=row_spec, check_vma=False)
```

```python
import jax
import jax.numpy as jnp
from jax import lax
from jax.experimental import pallas as pl
from jax.experimental.pallas import tpu as pltpu
from jax.sharding import PartitionSpec as P

MESH = pl.DeviceIdType.MESH
BF, F32 = jnp.bfloat16, jnp.float32
TOK, HID, FF, NE, NDEV = 256, 2048, 1408, 4, 16
CAP = 96
PER = 384
SLOTS = NDEV * CAP
WIN = 128
CW = 256
NC = HID // CW
PARTS = ((0, 96), (96, 80), (176, 80))
FULL = slice(None)


def layer_kernel(x_hbm, meta_ref, w1_hbm, w3_hbm, w2_hbm, out_hbm,
                 x_all, acc_a, acc_b, h_act, og, w13, w2b, xres, st0, st1, st2,
                 l1_ref, l2_ref, t_ref, gp_ref, meta, mrow, crow, at_rows, split, rslot, colq, st_ref,
                 ag_send, ag_recv, rs_send, rs_recv, d_send, d_recv, w13_sem, w2_sem, loc_sem, m_send, m_recv, credit):
    slots = h_act.at[:, 2 * CW:3 * CW]
    sgate = h_act.at[:, 3 * CW:3 * CW + 128]
    ez, ey, ex = lax.axis_index("ez"), lax.axis_index("ey"), lax.axis_index("ex")
    core = ex % 2
    pos = (ex // 2, ey, ez)

    def device(p, c):
        return (p[2], p[1], p[0] * 2 + c)

    def nbr(axis):
        p = list(pos)
        p[axis] = 1 - p[axis]
        return device(p, core)

    partner = device(pos, 1 - core)

    def cols(h):
        return pl.ds(pl.multiple_of(h * CW, CW), CW)

    def blocks(sel, c, rows, h):
        return x_all.at[sel[2], sel[1], sel[0], c, rows, cols(h)]

    def rows_of(k):
        return pl.ds(PARTS[k][0], PARTS[k][1])

    def pick(k, full, flip=()):
        sel = []
        for axis in range(3):
            if axis in full:
                sel.append(FULL)
            else:
                sel.append(1 - pos[axis] if axis in flip else pos[axis])
        return sel

    def ag(h, k, kind):
        a = [(k + i) % 3 for i in range(3)]
        if kind == 3:
            ref, to = blocks(pick(k, (a[0], a[1])), core, rows_of(k), h), partner
        elif kind == 4:
            ref, to = blocks(pick(k, (a[0], a[1]), (a[2],)), core, rows_of(k), h), partner
        else:
            ref, to = blocks(pick(k, tuple(a[:kind])), core, rows_of(k), h), nbr(a[kind])
        return pltpu.make_async_remote_copy(ref, ref, ag_send.at[h, k, kind], ag_recv.at[h, k, kind], device_id=to, device_id_type=MESH)

    def rs(h, k, kind):
        a = [(k + 2 - i) % 3 for i in range(3)]
        free = tuple(a[kind + 1:])
        src = blocks(pick(k, free, (a[kind],)), core, rows_of(k), h)
        if kind == 0:
            dst = st0.at[h % 2, :, :, rows_of(k), :]
        elif kind == 1:
            dst = st1.at[h % 2, :, rows_of(k), :]
        else:
            dst = st2.at[h % 2, rows_of(k), :]
        return pltpu.make_async_remote_copy(src, dst, rs_send.at[h, k, kind], rs_recv.at[h, k, kind], device_id=nbr(a[kind]), device_id_type=MESH)

    def cross(h):
        ref = blocks((FULL, FULL, FULL), 1 - core, FULL, h)
        return pltpu.make_async_remote_copy(ref, ref, d_send.at[h], d_recv.at[h], device_id=partner, device_id_type=MESH)

    def w13_copy(i, j):
        e, g = i % NE, i // NE
        src = (w1_hbm, w3_hbm)[j].at[e, pl.ds(pl.multiple_of(g * 2 * CW, 2 * CW), 2 * CW), :]
        return pltpu.make_async_copy(src, w13.at[i % 2, j], w13_sem.at[i % 2, j])

    def w2_copy(i):
        e, h = i % NE, i // NE
        return pltpu.make_async_copy(w2_hbm.at[e, :, cols(h)], w2b.at[i % 4], w2_sem.at[i % 4])

    me = ez * 8 + ey * 4 + ex

    def meta_copy(i):
        to = (me + i) % NDEV
        return pltpu.make_async_remote_copy(meta_ref.at[to], meta.at[me], m_send.at[i], m_recv.at[i],
                                            device_id=(to // 8, (to // 4) % 2, to % 4), device_id_type=MESH)

    def meta_from(i):
        src = (me + NDEV - i) % NDEV
        return pltpu.make_async_remote_copy(meta_ref.at[0], meta.at[src], m_send.at[i], m_recv.at[i],
                                            device_id=(0, 0, 0), device_id_type=MESH)

    own = pltpu.make_async_copy(x_hbm, x_all.at[pos[2], pos[1], pos[0], core], loc_sem.at[0])
    own.start()
    res = pltpu.make_async_copy(x_hbm, xres, loc_sem.at[1])
    res.start()
    for j in range(2):
        w13_copy(0, j).start()

    barrier = pltpu.get_barrier_semaphore()
    for i in range(1, NDEV):
        to = (me + i) % NDEV
        pl.semaphore_signal(barrier, inc=1, device_id=(to // 8, (to // 4) % 2, to % 4), device_id_type=MESH)
    own.wait()
    pl.semaphore_wait(barrier, NDEV - 1)
    for i in range(1, NDEV):
        meta_copy(i).start()

    def start(h, kind):
        for k in range(3):
            ag(h, k, kind).start()

    def arrive(h, kind):
        for k in range(3):
            ag(h, k, kind).wait_recv()

    for h in range(4):
        start(h, 0)

    def zero(i, _):
        acc_a[pl.ds(i * 128, 128), :] = jnp.zeros((128, FF), F32)
        acc_b[pl.ds(i * 128, 128), :] = jnp.zeros((128, FF), F32)
        return 0
    lax.fori_loop(0, NE * PER // 128, zero, 0)

    for h in range(2):
        arrive(h, 0)
        start(h, 1)

    meta[me] = meta_ref[me]
    for i in range(1, NDEV):
        meta_from(i).wait_recv()

    def times_t(lhs, rhs):
        return lax.dot_general(lhs, rhs, (((1,), (1,)), ((), ())), preferred_element_type=F32)

    for s in range(NDEV):
        g = meta[s]
        m = jnp.where(g > 0.0, 1.0, 0.0)
        mrow[s * 8:s * 8 + 8, :] = jnp.concatenate([m, jnp.max(m, axis=0, keepdims=True), jnp.zeros((3, TOK), F32)], axis=0)
        g1 = g.astype(BF).astype(F32)
        g2 = (g - g1).astype(BF).astype(F32)
        g3 = g - g1 - g2
        split[s] = jnp.concatenate([g1, g2, g3, jnp.zeros((4, TOK), F32)], axis=0).astype(BF)
    c = mrow[...]
    lane = lax.broadcasted_iota(jnp.int32, c.shape, 1)
    for n in range(8):
        c = c + jnp.where(lane >= 2 ** n, pltpu.roll(c, 2 ** n, 1), 0.0)
    crow[...] = c

    base = jnp.zeros((8, 1), F32)
    pieces = []
    for s in range(NDEV):
        m, c = mrow[s * 8:s * 8 + 8, :], crow[s * 8:s * 8 + 8, :]
        has = m > 0.5
        begin = jnp.minimum(jnp.floor(base * (1 / 16)) * 16, float(PER - WIN))
        at_rows[s * 8:s * 8 + 8, :] = jnp.where(has, base + c - begin, 0.0)
        rank = jnp.where(has, base + c, 0.0)
        high = jnp.floor(rank * (1 / 128))
        spot = lax.broadcasted_iota(jnp.int32, (CAP, TOK), 0).astype(F32)
        l1 = jnp.where(jnp.where(has, c, 0.0)[4:5, :] == spot + 1.0, 1.0, 0.0).astype(BF)
        l1_ref[s] = l1
        both = jnp.concatenate([rank - 128 * high, high], axis=0).astype(BF)
        got = times_t(both, l1)
        pieces.append(got[0:8, :] + 128 * got[8:16, :])
        if s % 4 == 3:
            rslot[:, (s // 4) * 4 * CAP:(s // 4 + 1) * 4 * CAP] = jnp.concatenate(pieces, axis=1)
            pieces = []
        for e in range(NE):
            st_ref[s * NE + e] = jnp.clip(jnp.sum(begin[e:e + 1, :]).astype(jnp.int32) // 16, 0, (PER - WIN) // 16) + e * (PER // 16)
        base = base + c[:, TOK - 1:TOK]
    eye = (lax.broadcasted_iota(jnp.int32, (TOK, TOK), 0) == lax.broadcasted_iota(jnp.int32, (TOK, TOK), 1))
    colq[...] = times_t(jnp.where(eye, 1.0, 0.0).astype(BF), at_rows[...].astype(BF))

    def fill_l2(b, _):
        for e in range(NE):
            p = lax.broadcasted_iota(jnp.int32, (32, SLOTS), 0) + (b * 32 + 1)
            l2_ref[pl.ds(pl.multiple_of(e * PER + b * 32, 32), 32), :] = jnp.where(rslot[e:e + 1, :] == p.astype(F32), 1.0, 0.0).astype(BF)
        return 0
    lax.fori_loop(0, PER // 32, fill_l2, 0)

    def gate_rows():
        for s in range(NDEV):
            got = times_t(l1_ref[s], split[s])
            sgate[s * CAP:(s + 1) * CAP, :] = jnp.concatenate([got, jnp.zeros((CAP, 112), F32)], axis=1).astype(BF)

        for e in range(NE):
            rows = slice(e * PER, (e + 1) * PER)
            got = jnp.dot(l2_ref[rows, :], sgate[...], preferred_element_type=F32)
            gp_ref[rows, :] = got[:, e:e + 1] + got[:, NE + e:NE + e + 1] + got[:, 2 * NE + e:2 * NE + e + 1]

    def fill_t(s):
        q = pltpu.roll(colq[...], 128 - s * 8, 1)
        place = lax.broadcasted_iota(jnp.int32, (TOK, WIN), 1).astype(F32) + 1.0
        t_ref[s] = jnp.concatenate([jnp.where(q[:, e:e + 1] == place, 1.0, 0.0).astype(BF) for e in range(NE)], axis=1)

    def compact(h):
        for s in range(NDEV):
            blk = x_all[s // 8, (s // 4) % 2, (s // 2) % 2, s % 2, :, cols(h)]
            slots[s * CAP:(s + 1) * CAP, :] = jnp.dot(l1_ref[s], blk, preferred_element_type=F32).astype(BF)

    def pack(h):
        def body(n, _):
            for e in range(2):
                rows = pl.ds(pl.multiple_of((2 * n + e) * PER, PER), PER)
                h_act[rows, pl.ds(pl.multiple_of((h % 2) * CW, CW), CW)] = jnp.dot(l2_ref[rows, :], slots[...], preferred_element_type=F32).astype(BF)
            return 0
        lax.fori_loop(0, NE // 2, body, 0)

    def expert_in(g, e):
        i = g * NE + e
        for j in range(2):
            w13_copy(i, j).wait()

        @pl.when(i + 1 < NC // 2 * NE)
        def _():
            for j in range(2):
                w13_copy(i + 1, j).start()

        rows = pl.ds(pl.multiple_of(e * PER, PER), PER)
        xe = h_act[rows, :2 * CW]
        acc_a[rows, :] += jnp.dot(xe, w13[i % 2, 0], preferred_element_type=F32)
        acc_b[rows, :] += jnp.dot(xe, w13[i % 2, 1], preferred_element_type=F32)

    def experts_in(g):
        def body(e, _):
            expert_in(g, e)
            return 0
        lax.fori_loop(0, NE, body, 0)

    def step_in(h, _):
        @pl.when(h < NC)
        def _():
            arrive(h, 1)
            start(h, 2)
            start(h, 3)

        @pl.when(h >= 1)
        def _():
            arrive(h - 1, 3)
            arrive(h - 1, 4)
            compact(h - 1)
            pack(h - 1)

        @pl.when(h + 2 < NC)
        def _():
            arrive(h + 2, 0)
            start(h + 2, 1)

        @pl.when(h + 4 < NC)
        def _():
            start(h + 4, 0)

        @pl.when(jnp.logical_and(h >= 1, h % 2 == 0))
        def _():
            experts_in((h - 1) // 2)

        @pl.when(h < NC)
        def _():
            fill_t(2 * h)
            fill_t(2 * h + 1)

        @pl.when(h < NC)
        def _():
            arrive(h, 2)
            start(h, 4)
        return 0

    lax.fori_loop(0, NC + 1, step_in, 0)
    gate_rows()

    def drain(h, _):
        for k in range(3):
            for kind in range(5):
                ag(h, k, kind).wait_send()
        return 0
    lax.fori_loop(0, NC, drain, 0)
    for i in range(1, NDEV):
        meta_copy(i).wait_send()
    pl.semaphore_signal(credit, inc=1, device_id=partner, device_id_type=MESH)
    for i in range(2):
        w2_copy(i).start()

    def activate(i, _):
        rows = pl.ds(pl.multiple_of(i * 32, 32), 32)
        a = acc_a[rows, :]
        h_act[rows, :] = (a * jax.nn.sigmoid(a) * acc_b[rows, :]).astype(BF)
        return 0
    lax.fori_loop(0, NE * PER // 32, activate, 0)
    res.wait()

    def expert_out(h):
        def body(n, _):
            i = h * NE + 2 * n
            w2_copy(i).wait()
            w2_copy(i + 1).wait()

            @pl.when(i + 2 < NC * NE)
            def _():
                w2_copy(i + 2).start()
                w2_copy(i + 3).start()
            for e in range(2):
                rows = pl.ds(pl.multiple_of((2 * n + e) * PER, PER), PER)
                o = jnp.dot(h_act[rows, :], w2b[(i + e) % 4], preferred_element_type=F32) * gp_ref[rows, :]
                high = o.astype(BF)
                tiles = pl.ds((2 * n + e) * (PER // 16), PER // 16)
                og[0, tiles] = high.reshape(PER // 16, 16, CW)
                og[1, tiles] = (o - high.astype(F32)).astype(BF).reshape(PER // 16, 16, CW)
            return 0
        lax.fori_loop(0, NE // 2, body, 0)

    def spread(s):
        total = None
        for half in range(2):
            rhs = jnp.concatenate([og[half, pl.ds(st_ref[s * NE + e], WIN // 16)].reshape(WIN, CW) for e in range(NE)], axis=0)
            part = jnp.dot(t_ref[s], rhs, preferred_element_type=F32)
            total = part if total is None else total + part
        return total

    def spread_all(h, c, plus):
        def body(j, _):
            for n in range(4):
                idx = (j, n // 2, n % 2, c, FULL, cols(h))
                total = spread((j * 4 + n) * 2 + c)
                if plus:
                    total = total + x_all[idx].astype(F32)
                x_all[idx] = total.astype(BF)
            return 0
        lax.fori_loop(0, 2, body, 0)

    def spread_other(h):
        spread_all(h, 1 - core, False)

    def spread_mine(h):
        spread_all(h, core, True)

    def add_in(h, kind):
        for k in range(3):
            rs(h, k, kind).wait_recv()
            a = [(k + 2 - i) % 3 for i in range(3)]
            free = a[kind + 1:]
            rows = rows_of(k)
            if kind == 2:
                sel = pos
                mine = x_all[sel[2], sel[1], sel[0], core, rows, cols(h)].astype(F32) + st2[h % 2, rows, :].astype(F32)
                xres[rows, cols(h)] = (xres[rows, cols(h)].astype(F32) + mine).astype(BF)
                continue
            order = sorted(free, reverse=True)
            for n in range(2 ** len(order)):
                sel = list(pos)
                bits = [(n >> (len(order) - 1 - b)) & 1 for b in range(len(order))]
                for axis, bit in zip(order, bits):
                    sel[axis] = bit
                got = st0[h % 2, bits[0], bits[1], rows, :] if kind == 0 else st1[h % 2, bits[0], rows, :]
                idx = (sel[2], sel[1], sel[0], core, rows, cols(h))
                x_all[idx] = (x_all[idx].astype(F32) + got.astype(F32)).astype(BF)

    def step_out(h, _):
        @pl.when(h < NC)
        def _():
            expert_out(h)
            spread_other(h)

            @pl.when(h == 0)
            def _():
                pl.semaphore_wait(credit, 1)
            cross(h).start()

        @pl.when(jnp.logical_and(h >= 1, h < NC + 1))
        def _():
            add_in(h - 1, 0)
            for k in range(3):
                rs(h - 1, k, 1).start()

        @pl.when(h < NC)
        def _():
            cross(h).wait_recv()
            spread_mine(h)
            for k in range(3):
                rs(h, k, 0).start()

        @pl.when(jnp.logical_and(h >= 1, h < NC + 1))
        def _():
            add_in(h - 1, 1)
            for k in range(3):
                rs(h - 1, k, 2).start()

        @pl.when(h >= 2)
        def _():
            add_in(h - 2, 2)
        return 0

    lax.fori_loop(0, NC + 2, step_out, 0)

    def drain_out(h, _):
        for k in range(3):
            for kind in range(3):
                rs(h, k, kind).wait_send()
        cross(h).wait_send()
        return 0
    lax.fori_loop(0, NC, drain_out, 0)
    fin = pltpu.make_async_copy(xres, out_hbm, loc_sem.at[0])
    fin.start()
    fin.wait()


def route(ids, gates):
    match = ids.T[None, :, :] == jnp.arange(NDEV * NE)[:, None, None]
    return jnp.sum(jnp.where(match, gates.T[None, :, :], 0.0), axis=1).reshape(NDEV, NE, TOK)


def solution(mesh):
    ep_axes = tuple(mesh.axis_names)
    row_spec, w_spec = P(ep_axes, None), P(ep_axes, None, None)
    vmem, anyspace = pl.BlockSpec(memory_space=pltpu.VMEM), pl.BlockSpec(memory_space=pl.ANY)

    def local_layer(tokens, ids, gates, w1, w3, w2):
        return pl.pallas_call(
            layer_kernel,
            name="moe_layer",
            out_shape=jax.ShapeDtypeStruct((TOK, HID), BF),
            in_specs=[anyspace, vmem, anyspace, anyspace, anyspace],
            out_specs=anyspace,
            scratch_shapes=[
                pltpu.VMEM((2, 2, 2, 2, TOK, HID), BF),
                pltpu.VMEM((NE * PER, FF), F32),
                pltpu.VMEM((NE * PER, FF), F32),
                pltpu.VMEM((NE * PER, FF), BF),
                pltpu.VMEM((2, NE * PER // 16, 16, CW), BF),
                pltpu.VMEM((2, 2, 2 * CW, FF), BF),
                pltpu.VMEM((4, FF, CW), BF),
                pltpu.VMEM((TOK, HID), BF),
                pltpu.VMEM((2, 2, 2, TOK, CW), BF),
                pltpu.VMEM((2, 2, TOK, CW), BF),
                pltpu.VMEM((2, TOK, CW), BF),
                pltpu.VMEM((NDEV, CAP, TOK), BF),
                pltpu.VMEM((NE * PER, SLOTS), BF),
                pltpu.VMEM((NDEV, TOK, NE * WIN), BF),
                pltpu.VMEM((NE * PER, 1), F32),
                pltpu.VMEM((NDEV, NE, TOK), F32),
                pltpu.VMEM((NDEV * 8, TOK), F32),
                pltpu.VMEM((NDEV * 8, TOK), F32),
                pltpu.VMEM((NDEV * 8, TOK), F32),
                pltpu.VMEM((NDEV, 4 * NE, TOK), BF),
                pltpu.VMEM((8, SLOTS), F32),
                pltpu.VMEM((TOK, 128), F32),
                pltpu.SMEM((NDEV * NE,), jnp.int32),
                pltpu.SemaphoreType.DMA((NC, 3, 5)),
                pltpu.SemaphoreType.DMA((NC, 3, 5)),
                pltpu.SemaphoreType.DMA((NC, 3, 3)),
                pltpu.SemaphoreType.DMA((NC, 3, 3)),
                pltpu.SemaphoreType.DMA((NC,)),
                pltpu.SemaphoreType.DMA((NC,)),
                pltpu.SemaphoreType.DMA((2, 2)),
                pltpu.SemaphoreType.DMA((4,)),
                pltpu.SemaphoreType.DMA((2,)),
                pltpu.SemaphoreType.DMA((NDEV,)),
                pltpu.SemaphoreType.DMA((NDEV,)),
                pltpu.SemaphoreType.REGULAR,
            ],
            compiler_params=pltpu.CompilerParams(collective_id=0, has_side_effects=True, vmem_limit_bytes=67_043_328),
        )(tokens, route(ids, gates), w1, w3, w2)

    return jax.shard_map(local_layer, mesh=mesh, in_specs=(row_spec, row_spec, row_spec, w_spec, w_spec, w_spec), out_specs=row_spec, check_vma=False)
```

```python
import jax
import jax.numpy as jnp
from jax import lax
from jax.experimental import pallas as pl
from jax.experimental.pallas import tpu as pltpu
from jax.sharding import PartitionSpec as P

MESH = pl.DeviceIdType.MESH
BF, F32 = jnp.bfloat16, jnp.float32
TOK, HID, FF, NE, NDEV = 256, 2048, 1408, 4, 16
CAP = 96
PER = 384
SLOTS = NDEV * CAP
WIN = 128
CW = 256
NC = HID // CW
PARTS = ((0, 96), (96, 80), (176, 80))
FULL = slice(None)


def layer_kernel(x_hbm, meta_ref, w1_hbm, w3_hbm, w2_hbm, out_hbm,
                 x_all, acc_a, acc_b, h_act, og, w13, w2b, xres,
                 l1_ref, l2_ref, t_ref, gp_ref, meta, mrow, crow, at_rows, split, rslot, colq, st_ref,
                 ag_send, ag_recv, rs_send, rs_recv, d_send, d_recv, w13_sem, w2_sem, loc_sem, m_send, m_recv, credit):
    slots = h_act.at[:, 2 * CW:4 * CW]
    sgate = h_act.at[:, 4 * CW:4 * CW + 128]
    ez, ey, ex = lax.axis_index("ez"), lax.axis_index("ey"), lax.axis_index("ex")
    core = ex % 2
    pos = (ex // 2, ey, ez)

    def device(p, c):
        return (p[2], p[1], p[0] * 2 + c)

    def nbr(axis):
        p = list(pos)
        p[axis] = 1 - p[axis]
        return device(p, core)

    partner = device(pos, 1 - core)

    def cols(h):
        return pl.ds(pl.multiple_of(h * CW, CW), CW)

    def blocks(sel, c, rows, h):
        return x_all.at[sel[2], sel[1], sel[0], c, rows, cols(h)]

    def rows_of(k):
        return pl.ds(PARTS[k][0], PARTS[k][1])

    def pick(k, full, flip=()):
        sel = []
        for axis in range(3):
            if axis in full:
                sel.append(FULL)
            else:
                sel.append(1 - pos[axis] if axis in flip else pos[axis])
        return sel

    def ag(h, k, kind):
        a = [(k + i) % 3 for i in range(3)]
        if kind == 3:
            ref, to = blocks(pick(k, (a[0], a[1])), core, rows_of(k), h), partner
        elif kind == 4:
            ref, to = blocks(pick(k, (a[0], a[1]), (a[2],)), core, rows_of(k), h), partner
        else:
            ref, to = blocks(pick(k, tuple(a[:kind])), core, rows_of(k), h), nbr(a[kind])
        return pltpu.make_async_remote_copy(ref, ref, ag_send.at[h, k, kind], ag_recv.at[h, k, kind], device_id=to, device_id_type=MESH)

    def landing(h, k, kind):
        sel = [FULL] * 3
        for i in range(kind + 1):
            sel[(k + 2 - i) % 3] = 0 if i == kind else 1
        return (sel[2], sel[1], sel[0], 1 - core, rows_of(k), cols((h + NC - 3) % NC))

    def rs(h, k, kind):
        a = [(k + 2 - i) % 3 for i in range(3)]
        src = blocks(pick(k, tuple(a[kind + 1:]), (a[kind],)), core, rows_of(k), h)
        return pltpu.make_async_remote_copy(src, x_all.at[landing(h, k, kind)], rs_send.at[h, k, kind], rs_recv.at[h, k, kind],
                                            device_id=nbr(a[kind]), device_id_type=MESH)

    def cross(h):
        ref = blocks((FULL, FULL, FULL), 1 - core, FULL, h)
        return pltpu.make_async_remote_copy(ref, ref, d_send.at[h], d_recv.at[h], device_id=partner, device_id_type=MESH)

    def w13_copy(i, j):
        e, g = i % NE, i // NE
        src = (w1_hbm, w3_hbm)[j].at[e, pl.ds(pl.multiple_of(g * 2 * CW, 2 * CW), 2 * CW), :]
        return pltpu.make_async_copy(src, w13.at[i % 2, j], w13_sem.at[i % 2, j])

    def w2_copy(i):
        e, h = i % NE, i // NE
        return pltpu.make_async_copy(w2_hbm.at[e, :, cols(h)], w2b.at[i % 6], w2_sem.at[i % 6])

    me = ez * 8 + ey * 4 + ex

    def meta_copy(i):
        to = (me + i) % NDEV
        return pltpu.make_async_remote_copy(meta_ref.at[to], meta.at[me], m_send.at[i], m_recv.at[i],
                                            device_id=(to // 8, (to // 4) % 2, to % 4), device_id_type=MESH)

    def meta_from(i):
        src = (me + NDEV - i) % NDEV
        return pltpu.make_async_remote_copy(meta_ref.at[0], meta.at[src], m_send.at[i], m_recv.at[i],
                                            device_id=(0, 0, 0), device_id_type=MESH)

    own = pltpu.make_async_copy(x_hbm, x_all.at[pos[2], pos[1], pos[0], core], loc_sem.at[0])
    own.start()
    res = pltpu.make_async_copy(x_hbm, xres, loc_sem.at[1])
    res.start()
    for j in range(2):
        w13_copy(0, j).start()

    barrier = pltpu.get_barrier_semaphore()
    for i in range(1, NDEV):
        to = (me + i) % NDEV
        pl.semaphore_signal(barrier, inc=1, device_id=(to // 8, (to // 4) % 2, to % 4), device_id_type=MESH)
    own.wait()
    pl.semaphore_wait(barrier, NDEV - 1)
    for i in range(1, NDEV):
        meta_copy(i).start()

    def start(h, kind):
        for k in range(3):
            ag(h, k, kind).start()

    def arrive(h, kind):
        for k in range(3):
            ag(h, k, kind).wait_recv()

    def service(h):
        arrive(h, 1)
        start(h, 2)
        start(h, 3)

        @pl.when(h + 2 < NC)
        def _():
            arrive(h + 2, 0)
            start(h + 2, 1)

        @pl.when(h + 4 < NC)
        def _():
            start(h + 4, 0)

    for h in range(4):
        start(h, 0)

    def zero(i, _):
        acc_a[pl.ds(i * 128, 128), :] = jnp.zeros((128, FF), F32)
        acc_b[pl.ds(i * 128, 128), :] = jnp.zeros((128, FF), F32)
        return 0
    lax.fori_loop(0, NE * PER // 128, zero, 0)

    for h in range(2):
        arrive(h, 0)
        start(h, 1)

    meta[me] = meta_ref[me]
    for i in range(1, NDEV):
        meta_from(i).wait_recv()

    def times_t(lhs, rhs):
        return lax.dot_general(lhs, rhs, (((1,), (1,)), ((), ())), preferred_element_type=F32)

    for s in range(NDEV):
        g = meta[s]
        m = jnp.where(g > 0.0, 1.0, 0.0)
        mrow[s * 8:s * 8 + 8, :] = jnp.concatenate([m, jnp.max(m, axis=0, keepdims=True), jnp.zeros((3, TOK), F32)], axis=0)
        g1 = g.astype(BF).astype(F32)
        g2 = (g - g1).astype(BF).astype(F32)
        g3 = g - g1 - g2
        split[s] = jnp.concatenate([g1, g2, g3, jnp.zeros((4, TOK), F32)], axis=0).astype(BF)
    service(0)
    c = mrow[...]
    lane = lax.broadcasted_iota(jnp.int32, c.shape, 1)
    for n in range(8):
        c = c + jnp.where(lane >= 2 ** n, pltpu.roll(c, 2 ** n, 1), 0.0)
    crow[...] = c

    base = jnp.zeros((8, 1), F32)
    pieces = []
    for s in range(NDEV):
        m, c = mrow[s * 8:s * 8 + 8, :], crow[s * 8:s * 8 + 8, :]
        has = m > 0.5
        begin = jnp.minimum(jnp.floor(base * (1 / 16)) * 16, float(PER - WIN))
        at_rows[s * 8:s * 8 + 8, :] = jnp.where(has, base + c - begin, 0.0)
        rank = jnp.where(has, base + c, 0.0)
        high = jnp.floor(rank * (1 / 128))
        spot = lax.broadcasted_iota(jnp.int32, (CAP, TOK), 0).astype(F32)
        l1 = jnp.where(jnp.where(has, c, 0.0)[4:5, :] == spot + 1.0, 1.0, 0.0).astype(BF)
        l1_ref[s] = l1
        both = jnp.concatenate([rank - 128 * high, high], axis=0).astype(BF)
        got = times_t(both, l1)
        pieces.append(got[0:8, :] + 128 * got[8:16, :])
        if s % 4 == 3:
            rslot[:, (s // 4) * 4 * CAP:(s // 4 + 1) * 4 * CAP] = jnp.concatenate(pieces, axis=1)
            pieces = []
        for e in range(NE):
            st_ref[s * NE + e] = jnp.clip(jnp.sum(begin[e:e + 1, :]).astype(jnp.int32) // 16, 0, (PER - WIN) // 16) + e * (PER // 16)
        base = base + c[:, TOK - 1:TOK]
    eye = (lax.broadcasted_iota(jnp.int32, (TOK, TOK), 0) == lax.broadcasted_iota(jnp.int32, (TOK, TOK), 1))
    colq[...] = times_t(jnp.where(eye, 1.0, 0.0).astype(BF), at_rows[...].astype(BF))

    def fill_l2(b, _):
        for e in range(NE):
            p = lax.broadcasted_iota(jnp.int32, (32, SLOTS), 0) + (b * 32 + 1)
            l2_ref[pl.ds(pl.multiple_of(e * PER + b * 32, 32), 32), :] = jnp.where(rslot[e:e + 1, :] == p.astype(F32), 1.0, 0.0).astype(BF)
        return 0
    lax.fori_loop(0, PER // 32, fill_l2, 0)

    def gate_rows():
        for s in range(NDEV):
            got = times_t(l1_ref[s], split[s])
            sgate[s * CAP:(s + 1) * CAP, :] = jnp.concatenate([got, jnp.zeros((CAP, 112), F32)], axis=1).astype(BF)

        for e in range(NE):
            rows = slice(e * PER, (e + 1) * PER)
            got = jnp.dot(l2_ref[rows, :], sgate[...], preferred_element_type=F32)
            gp_ref[rows, :] = got[:, e:e + 1] + got[:, NE + e:NE + e + 1] + got[:, 2 * NE + e:2 * NE + e + 1]

    def fill_t(s):
        q = pltpu.roll(colq[...], 128 - s * 8, 1)
        place = lax.broadcasted_iota(jnp.int32, (TOK, WIN), 1).astype(F32) + 1.0
        t_ref[s] = jnp.concatenate([jnp.where(q[:, e:e + 1] == place, 1.0, 0.0).astype(BF) for e in range(NE)], axis=1)

    def compact(h):
        c = pl.ds(pl.multiple_of((h % 2) * CW, CW), CW)
        for s in range(NDEV):
            blk = x_all[s // 8, (s // 4) % 2, (s // 2) % 2, s % 2, :, cols(h)]
            slots[s * CAP:(s + 1) * CAP, c] = jnp.dot(l1_ref[s], blk, preferred_element_type=F32).astype(BF)

    def pack():
        def body(e, _):
            rows = pl.ds(pl.multiple_of(e * PER, PER), PER)
            h_act[rows, :2 * CW] = jnp.dot(l2_ref[rows, :], slots[...], preferred_element_type=F32).astype(BF)
            return 0
        lax.fori_loop(0, NE, body, 0)

    def expert_in(g, e):
        i = g * NE + e
        for j in range(2):
            w13_copy(i, j).wait()

        @pl.when(i + 1 < NC // 2 * NE)
        def _():
            for j in range(2):
                w13_copy(i + 1, j).start()

        rows = pl.ds(pl.multiple_of(e * PER, PER), PER)
        xe = h_act[rows, :2 * CW]
        acc_a[rows, :] += jnp.dot(xe, w13[i % 2, 0], preferred_element_type=F32)
        acc_b[rows, :] += jnp.dot(xe, w13[i % 2, 1], preferred_element_type=F32)

    def experts_in(g, lo, hi):
        def body(e, _):
            expert_in(g, e)
            return 0
        lax.fori_loop(lo, hi, body, 0)

    def step_in(h, _):
        arrive(h, 2)
        start(h, 4)

        @pl.when(h + 1 < NC)
        def _():
            service(h + 1)

        @pl.when(jnp.logical_and(h % 2 == 0, h >= 2))
        def _():
            experts_in(h // 2 - 1, 2, NE)
        fill_t(2 * h)
        fill_t(2 * h + 1)
        arrive(h, 3)
        arrive(h, 4)
        compact(h)

        @pl.when(h % 2 == 1)
        def _():
            pack()
            experts_in(h // 2, 0, 2)
        return 0

    lax.fori_loop(0, NC, step_in, 0)
    experts_in(NC // 2 - 1, 2, NE)
    gate_rows()

    def drain(h, _):
        for k in range(3):
            for kind in range(5):
                ag(h, k, kind).wait_send()
        return 0
    lax.fori_loop(0, NC, drain, 0)
    for i in range(1, NDEV):
        meta_copy(i).wait_send()
    for to in (nbr(0), nbr(1), nbr(2), partner):
        pl.semaphore_signal(credit, inc=1, device_id=to, device_id_type=MESH)
    for i in range(4):
        w2_copy(i).start()

    def activate(i, _):
        rows = pl.ds(pl.multiple_of(i * 32, 32), 32)
        a = acc_a[rows, :]
        h_act[rows, :] = (a * jax.nn.sigmoid(a) * acc_b[rows, :]).astype(BF)
        return 0
    lax.fori_loop(0, NE * PER // 32, activate, 0)
    res.wait()

    def expert_out(h):
        def body(n, _):
            i = h * NE + 2 * n
            w2_copy(i).wait()
            w2_copy(i + 1).wait()

            @pl.when(i + 4 < NC * NE)
            def _():
                w2_copy(i + 4).start()
                w2_copy(i + 5).start()
            for e in range(2):
                rows = pl.ds(pl.multiple_of((2 * n + e) * PER, PER), PER)
                o = jnp.dot(h_act[rows, :], w2b[(i + e) % 6], preferred_element_type=F32) * gp_ref[rows, :]
                high = o.astype(BF)
                tiles = pl.ds((2 * n + e) * (PER // 16), PER // 16)
                og[0, tiles] = high.reshape(PER // 16, 16, CW)
                og[1, tiles] = (o - high.astype(F32)).astype(BF).reshape(PER // 16, 16, CW)
            return 0
        lax.fori_loop(0, NE // 2, body, 0)

    def spread(s):
        total = None
        for half in range(2):
            rhs = jnp.concatenate([og[half, pl.ds(st_ref[s * NE + e], WIN // 16)].reshape(WIN, CW) for e in range(NE)], axis=0)
            part = jnp.dot(t_ref[s], rhs, preferred_element_type=F32)
            total = part if total is None else total + part
        return total

    def spread_all(h, c, plus):
        def body(j, _):
            for n in range(4):
                idx = (j, n // 2, n % 2, c, FULL, cols(h))
                total = spread((j * 4 + n) * 2 + c)
                if plus:
                    total = total + x_all[idx].astype(F32)
                x_all[idx] = total.astype(BF)
            return 0
        lax.fori_loop(0, 2, body, 0)

    def spread_other(h):
        spread_all(h, 1 - core, False)

    def spread_mine(h):
        spread_all(h, core, True)

    def add_in(h, kind):
        for k in range(3):
            rs(h, k, kind).wait_recv()
            rows = rows_of(k)
            land = landing(h, k, kind)
            order = [2 - i for i in range(3) if land[i] == FULL]
            for n in range(2 ** len(order)):
                sel, at = list(pos), list(land)
                for b, axis in enumerate(order):
                    bit = (n >> (len(order) - 1 - b)) & 1
                    sel[axis] = bit
                    at[2 - axis] = bit
                idx = (sel[2], sel[1], sel[0], core, rows, cols(h))
                total = x_all[idx].astype(F32) + x_all[tuple(at)].astype(F32)
                if kind == 2:
                    xres[rows, cols(h)] = (xres[rows, cols(h)].astype(F32) + total).astype(BF)
                else:
                    x_all[idx] = total.astype(BF)

    def hop(h, kind):
        for k in range(3):
            rs(h, k, kind).start()

    def step_out(h, _):
        @pl.when(h < NC)
        def _():
            expert_out(h)
            spread_other(h)

            @pl.when(h == 0)
            def _():
                pl.semaphore_wait(credit, 4)
            cross(h).start()

        @pl.when(h >= 3)
        def _():
            add_in(h - 3, 2)

        @pl.when(h < NC)
        def _():
            @pl.when(h >= 1)
            def _():
                cross(h - 1).wait_send()
            cross(h).wait_recv()
            spread_mine(h)
            hop(h, 0)

        @pl.when(jnp.logical_and(h >= 1, h < NC + 1))
        def _():
            add_in(h - 1, 0)
            hop(h - 1, 1)

        @pl.when(jnp.logical_and(h >= 2, h < NC + 2))
        def _():
            add_in(h - 2, 1)
            hop(h - 2, 2)
        return 0

    lax.fori_loop(0, NC + 3, step_out, 0)
    cross(NC - 1).wait_send()

    def drain_out(h, _):
        for k in range(3):
            for kind in range(3):
                rs(h, k, kind).wait_send()
        return 0
    lax.fori_loop(0, NC, drain_out, 0)
    fin = pltpu.make_async_copy(xres, out_hbm, loc_sem.at[0])
    fin.start()
    fin.wait()


def route(ids, gates):
    match = ids.T[None, :, :] == jnp.arange(NDEV * NE)[:, None, None]
    return jnp.sum(jnp.where(match, gates.T[None, :, :], 0.0), axis=1).reshape(NDEV, NE, TOK)


def solution(mesh):
    ep_axes = tuple(mesh.axis_names)
    row_spec, w_spec = P(ep_axes, None), P(ep_axes, None, None)
    vmem, anyspace = pl.BlockSpec(memory_space=pltpu.VMEM), pl.BlockSpec(memory_space=pl.ANY)

    def local_layer(tokens, ids, gates, w1, w3, w2):
        return pl.pallas_call(
            layer_kernel,
            name="moe_layer",
            out_shape=jax.ShapeDtypeStruct((TOK, HID), BF),
            in_specs=[anyspace, vmem, anyspace, anyspace, anyspace],
            out_specs=anyspace,
            scratch_shapes=[
                pltpu.VMEM((2, 2, 2, 2, TOK, HID), BF),
                pltpu.VMEM((NE * PER, FF), F32),
                pltpu.VMEM((NE * PER, FF), F32),
                pltpu.VMEM((NE * PER, FF), BF),
                pltpu.VMEM((2, NE * PER // 16, 16, CW), BF),
                pltpu.VMEM((2, 2, 2 * CW, FF), BF),
                pltpu.VMEM((6, FF, CW), BF),
                pltpu.VMEM((TOK, HID), BF),
                pltpu.VMEM((NDEV, CAP, TOK), BF),
                pltpu.VMEM((NE * PER, SLOTS), BF),
                pltpu.VMEM((NDEV, TOK, NE * WIN), BF),
                pltpu.VMEM((NE * PER, 1), F32),
                pltpu.VMEM((NDEV, NE, TOK), F32),
                pltpu.VMEM((NDEV * 8, TOK), F32),
                pltpu.VMEM((NDEV * 8, TOK), F32),
                pltpu.VMEM((NDEV * 8, TOK), F32),
                pltpu.VMEM((NDEV, 4 * NE, TOK), BF),
                pltpu.VMEM((8, SLOTS), F32),
                pltpu.VMEM((TOK, 128), F32),
                pltpu.SMEM((NDEV * NE,), jnp.int32),
                pltpu.SemaphoreType.DMA((NC, 3, 5)),
                pltpu.SemaphoreType.DMA((NC, 3, 5)),
                pltpu.SemaphoreType.DMA((NC, 3, 3)),
                pltpu.SemaphoreType.DMA((NC, 3, 3)),
                pltpu.SemaphoreType.DMA((NC,)),
                pltpu.SemaphoreType.DMA((NC,)),
                pltpu.SemaphoreType.DMA((2, 2)),
                pltpu.SemaphoreType.DMA((6,)),
                pltpu.SemaphoreType.DMA((2,)),
                pltpu.SemaphoreType.DMA((NDEV,)),
                pltpu.SemaphoreType.DMA((NDEV,)),
                pltpu.SemaphoreType.REGULAR,
            ],
            compiler_params=pltpu.CompilerParams(collective_id=0, has_side_effects=True, vmem_limit_bytes=67_043_328),
        )(tokens, route(ids, gates), w1, w3, w2)

    return jax.shard_map(local_layer, mesh=mesh, in_specs=(row_spec, row_spec, row_spec, w_spec, w_spec, w_spec), out_specs=row_spec, check_vma=False)
```
